32 devices in a mesh: left: 4 (over z), right: 8 (over y, x, core).
Axes of the slice: x: 2, y: 2, z: 4, core: 2. Of those that a mesh axis runs over, the one named last changes fastest.
Arguments:
- wavefunction: bfloat16 [5120, 5120], P('left', 'right'), may hold values from -6 to 6
- left_env: bfloat16 [8, 5120, 640], P(None, 'left'), may hold values from -0.25 to 0.25
- right_env: bfloat16 [8, 640, 5120], P(None, None, 'right'), may hold values from -0.25 to 0.25
- left_sizes: int32 [8], replicated, may hold values from 512 to 640, as said below
- right_sizes: int32 [8], replicated, may hold values from 512 to 640, as said below
- allowed: int32 [15], replicated, may hold values 0 or 1
- channel_shift: int32 [8], replicated, may hold values from -1 to 1, as said below
Outputs:
- evolved: bfloat16 [5120, 5120], P('left', 'right')
The draws below stay inside these ranges and needn't reach their ends.
Inputs may be any that keep to these rules, and one draw needn't show every extreme that they name: `left_sizes`: multiples of 128; in every draw some left sector has exactly 640. `right_sizes`: multiples of 128; in every draw some right sector has exactly 640. `channel_shift`: each of -1, 0 and 1 occurs.
All inputs are finite; a program needn't handle non-finite values.
Results may differ from the reference program's by a relative error of at most 0.0054.
Values may be sent and summed in bfloat16 or wider, within the bound.
No kernel may reach another device: no remote copies, remote signals or barrier semaphores. Data moves between devices by JAX's collectives and lax.ppermute only.
A program may use at most 192 MiB of HBM per device.

```python
import jax
import jax.numpy as jnp
from jax import lax

MAXS = 640
GRAIN = 128
CHANNELS = 8
STEPS = 2
LEFT_SECTORS = 8
RIGHT_SECTORS = 8
LEFT_ROWS = 5120
RIGHT_COLS = 5120


def draw_left_sizes(key, part):
    first_key, second_key = jax.random.split(key)
    grains = jax.random.randint(first_key, (LEFT_SECTORS,), MAXS // GRAIN - 1, MAXS // GRAIN + 1)
    widest = jax.random.randint(second_key, (), 0, LEFT_SECTORS)
    grains = jnp.where(jnp.arange(LEFT_SECTORS) == widest, MAXS // GRAIN, grains)
    return (grains * GRAIN).astype(jnp.int32)


def draw_right_sizes(key, part):
    first_key, second_key = jax.random.split(jax.random.fold_in(key, 7))
    grains = jax.random.randint(first_key, (RIGHT_SECTORS,), MAXS // GRAIN - 1, MAXS // GRAIN + 1)
    widest = jax.random.randint(second_key, (), 0, RIGHT_SECTORS)
    grains = jnp.where(jnp.arange(RIGHT_SECTORS) == widest, MAXS // GRAIN, grains)
    return (grains * GRAIN).astype(jnp.int32)


def draw_channel_shift(key, part):
    first_key, second_key = jax.random.split(jax.random.fold_in(key, 11))
    extra = jax.random.randint(first_key, (CHANNELS,), -1, 2)
    counter = jnp.arange(CHANNELS)
    base = jnp.where(counter < 3, counter - 1, extra)
    order = jax.random.permutation(second_key, CHANNELS)
    return base[order].astype(jnp.int32)


def set_ends(values, key, smallest, largest):
    index_at = [jax.random.randint(jax.random.fold_in(key, axis), (), 0, length) for axis, length in enumerate(values.shape)]
    widest = values.shape.index(max(values.shape))
    neighbour = index_at[:widest] + [(index_at[widest] + 1) % values.shape[widest]] + index_at[widest + 1:]
    return values.at[tuple(index_at)].set(smallest).at[tuple(neighbour)].set(largest)


def block_scale(rng, extent, cuts, least, largest):
    def one(position, blocks):
        steps = jax.random.uniform(jax.random.fold_in(jax.random.fold_in(rng, 6), position), (blocks,), jnp.float32, least / len(cuts), largest / len(cuts))
        return jnp.repeat(jnp.exp(steps), extent[position] // blocks).reshape((-1,) + (1,) * (len(extent) - position - 1))

    gain = one(*cuts[0])
    for cut in cuts[1:]:
        gain = gain * one(*cut)
    return gain


def scatter_about(rng, shape, scale, bound, cuts=(), kind=jnp.bfloat16):
    result = jax.random.normal(rng, shape, jnp.float32) * scale
    if len(cuts) > 0:
        result = block_scale(rng, shape, cuts, -0.22, 0.18) * result
    return jnp.clip(result, min=-bound, max=bound).astype(kind)


def setup_inputs(seed: int = 0) -> dict:
    keys = jax.random.split(jax.random.key(seed), 8)
    wavefunction = scatter_about(keys[0], (LEFT_ROWS, RIGHT_COLS), 1.0, 6.0, ((0, 4), (1, 8)))
    left_env = scatter_about(keys[1], (CHANNELS, LEFT_ROWS, MAXS), MAXS ** -0.5, 0.25, ((1, 4),))
    right_env = scatter_about(keys[2], (CHANNELS, MAXS, RIGHT_COLS), MAXS ** -0.5, 0.25, ((2, 8),))
    left_sizes = draw_left_sizes(jax.random.fold_in(keys[7], 71), 0)
    right_sizes = draw_right_sizes(jax.random.fold_in(keys[7], 71), 0)
    allowed = set_ends((jax.random.randint(keys[5], (LEFT_SECTORS + RIGHT_SECTORS - 1,), 0, 3) < 2).astype(jnp.int32), jax.random.fold_in(keys[5], 1), 0, 1)
    channel_shift = draw_channel_shift(jax.random.fold_in(keys[7], 71), 0)
    return {"wavefunction": wavefunction, "left_env": left_env, "right_env": right_env, "left_sizes": left_sizes, "right_sizes": right_sizes, "allowed": allowed, "channel_shift": channel_shift}


time_step = 0.5


def keep_factor(left_sizes, right_sizes, allowed):
    positions = jnp.arange(MAXS, dtype=jnp.int32)
    row_keep = (positions[None, :] < left_sizes[:, None]).astype(jnp.float32)
    col_keep = (positions[None, :] < right_sizes[:, None]).astype(jnp.float32)
    sector_left = jnp.arange(LEFT_SECTORS, dtype=jnp.int32)
    sector_right = jnp.arange(RIGHT_SECTORS, dtype=jnp.int32)
    blocks = allowed[sector_left[:, None] + sector_right[None, :]].astype(jnp.float32)
    return row_keep[:, :, None, None] * blocks[:, None, :, None] * col_keep[None, None, :, :]


def masked(values, factor):
    shaped = values.reshape(LEFT_SECTORS, MAXS, RIGHT_SECTORS, MAXS)
    return (shaped * factor).reshape(LEFT_ROWS, RIGHT_COLS)


def reference(wavefunction, left_env, right_env, left_sizes, right_sizes, allowed, channel_shift):
    factor = keep_factor(left_sizes, right_sizes, allowed)
    current = masked(wavefunction.astype(jnp.float32), factor).astype(jnp.bfloat16)
    for taylor_step in range(STEPS):
        slots = current.reshape(LEFT_SECTORS, MAXS, RIGHT_COLS)
        empty_rows = jnp.zeros((1, MAXS, RIGHT_COLS), jnp.bfloat16)
        padded = jnp.concatenate([empty_rows, slots, empty_rows], axis=0)
        applied = jnp.zeros((LEFT_ROWS, RIGHT_COLS), jnp.float32)
        for channel in range(CHANNELS):
            shift_now = channel_shift[channel]
            sources = lax.dynamic_slice_in_dim(padded, (1 - shift_now).astype(jnp.int32), LEFT_SECTORS, 0)
            blocks = left_env[channel].reshape(LEFT_SECTORS, MAXS, MAXS)
            partial_value = jnp.einsum("sik,skc->sic", blocks.astype(jnp.float32), sources.astype(jnp.float32))
            partial_value = partial_value.astype(jnp.bfloat16).reshape(LEFT_ROWS, RIGHT_SECTORS, MAXS)
            empty_cols = jnp.zeros((LEFT_ROWS, 1, MAXS), jnp.bfloat16)
            widened = jnp.concatenate([empty_cols, partial_value, empty_cols], axis=1)
            picked = lax.dynamic_slice_in_dim(widened, (1 + shift_now).astype(jnp.int32), RIGHT_SECTORS, 1)
            right_blocks = right_env[channel].reshape(MAXS, RIGHT_SECTORS, MAXS)
            term = jnp.einsum("rjk,kjc->rjc", picked.astype(jnp.float32), right_blocks.astype(jnp.float32))
            applied = applied + term.reshape(LEFT_ROWS, RIGHT_COLS)
        current = masked(current.astype(jnp.float32) - time_step * applied, factor).astype(jnp.bfloat16)
    return current
```

```python
import functools

import jax
import jax.numpy as jnp
from jax import lax
from jax.experimental import pallas as pl
from jax.experimental.pallas import tpu as pltpu
from jax.sharding import PartitionSpec as P

STEPS = 2
TIME_STEP = 0.5
AXES = ("left", "right")


def permute_pairs(rows, cols, even_move, odd_move):
    pairs = []
    for row in range(rows):
        for col in range(cols):
            down, across = odd_move if col % 2 else even_move
            to_row, to_col = row + down, col + across
            if 0 <= to_row < rows and 0 <= to_col < cols:
                pairs.append((row * cols + col, to_row * cols + to_col))
    return pairs


class Place:
    def __init__(self, sizes, stream):
        self.left_sizes, self.right_sizes, self.allowed, self.shift = sizes
        self.row = lax.axis_index("left")
        self.col = lax.axis_index("right")
        self.odd_col = lax.rem(self.col, 2)
        self.slot = self.odd_col if stream == "even" else 1 - self.odd_col
        self.sector = 2 * self.row + self.slot
        self.far_shift = 2 * self.odd_col - 1

    def is_allowed(self):
        return self.allowed[self.sector + self.col] == 1

    def keep(self, shape, shift):
        sector = jnp.clip(self.sector - shift, 0, self.left_sizes.shape[0] - 1)
        column = jnp.clip(self.col + shift, 0, self.right_sizes.shape[0] - 1)
        rows = lax.broadcasted_iota(jnp.int32, shape, 0) < self.left_sizes[sector]
        cols = lax.broadcasted_iota(jnp.int32, shape, 1) < self.right_sizes[column]
        return rows & cols

    def masked(self, value, shift):
        value = value.astype(jnp.float32)
        return jnp.where(self.keep(value.shape, shift), value, 0.0).astype(jnp.bfloat16)


class Tasks:
    def __init__(self, place, list_ref):
        self.shift = place.shift
        self.list = list_ref
        self.size = jnp.int32(0)
        groups = (0, -place.far_shift, place.far_shift)
        self.groups = []
        start = jnp.int32(0)
        for group in groups:
            count = lax.fori_loop(
                0, self.shift.shape[0], lambda w, n, g=group: n + (self.shift[w] == g).astype(jnp.int32), 0
            )
            self.groups.append((group, start, count))
            start = start + count

    def write_order(self, order_ref):
        for group, start, _ in self.groups:

            def place_one(w, at, group=group):
                @pl.when(self.shift[w] == group)
                def _():
                    order_ref[at] = w

                return at + (self.shift[w] == group).astype(jnp.int32)

            lax.fori_loop(0, self.shift.shape[0], place_one, start)

    def add(self, group, users):
        _, start, count = self.groups[group]

        def one(i, size):
            at = start + 2 * i
            for place, source, stream in users:
                wanted = place.is_allowed()

                @pl.when(wanted)
                def _(source=source, stream=stream, size=size):
                    self.list[0, size] = source
                    self.list[1, size] = stream
                    self.list[2, size] = at
                    self.list[3, size] = jnp.minimum(count - 2 * i, 2)

                size = size + wanted.astype(jnp.int32)
            return size

        self.size = lax.fori_loop(0, lax.div(count + 1, 2), one, self.size)


def add_channels(tasks, slots, sources, acc_ref, left_ref, right_ref, mixed_ref, fetch=None):
    maxs = right_ref.shape[0]
    wide = 2 * maxs
    tile = 256

    def run(i, ready):
        source, stream, at, length = (tasks.list[k, i] for k in range(4))
        if fetch is not None:
            lax.fori_loop(ready, at + length, fetch, None)
            ready = jnp.maximum(ready, at + length)
        rows = pl.ds(pl.multiple_of(jnp.where(stream == 0, slots[0], slots[1]) * maxs, maxs), maxs)
        begin = at * maxs

        def go(depth):
            for low in range(0, depth, tile):
                high = min(low + tile, depth)
                part = jnp.dot(
                    sources[source],
                    right_ref[:, pl.ds(pl.multiple_of(begin + low, 128), high - low)],
                    preferred_element_type=jnp.float32,
                ).astype(jnp.bfloat16)
                split = min(max(maxs, low), high)
                if split > low:
                    mixed_ref[0:maxs, low:split] = part[:, : split - low]
                if high > split:
                    mixed_ref[maxs:wide, split - maxs : high - maxs] = part[:, split - low :]
            for low in range(0, maxs, tile):
                high = min(low + tile, maxs)
                acc_ref[stream, :, low:high] += jnp.dot(
                    left_ref[rows, pl.ds(pl.multiple_of(begin, 128), depth)],
                    mixed_ref[0:depth, low:high],
                    preferred_element_type=jnp.float32,
                )

        @pl.when(length == 2)
        def _():
            go(wide)

        @pl.when(length == 1)
        def _():
            go(maxs)

        return ready

    return lax.fori_loop(0, tasks.size, run, jnp.int32(0))


def near_kernel(first, ls, rs, al, sh, xe, xo, near, left, right, acc, *rest):
    sizes = (ls, rs, al, sh)
    even, odd = Place(sizes, "even"), Place(sizes, "odd")
    if first:
        lcat, rcat, sources, mixed, list_ref, order, left_sem, right_sem = rest
    else:
        lcat, rcat = left, right
        sources, mixed, list_ref = rest
    maxs = rcat.shape[0]
    channels = sh.shape[0]
    tasks = Tasks(even, list_ref)
    fetch = None
    if first:
        tasks.write_order(order)

        def copies(at):
            w = order[at]
            cols = pl.ds(pl.multiple_of(at * maxs, 128), maxs)
            return (
                pltpu.make_async_copy(right.at[w], rcat.at[:, cols], right_sem.at[at]),
                pltpu.make_async_copy(left.at[w], lcat.at[:, cols], left_sem.at[at]),
            )

        def begin(at, _):
            for copy in copies(at):
                copy.start()

        def fetch(at, _):
            for copy in copies(at):
                copy.wait()

        lax.fori_loop(0, channels, begin, None)
        sources[0] = even.masked(xe[...], 0)
        sources[1] = odd.masked(xo[...], 0)
        sources[2] = odd.masked(near[...], -odd.far_shift)
    else:
        sources[0] = xe[...]
        sources[1] = xo[...]
        sources[2] = near[...]
    acc[...] = jnp.zeros_like(acc)
    tasks.add(0, ((even, 0, 0), (odd, 1, 1)))
    tasks.add(1, ((odd, 2, 1),))
    ready = add_channels(tasks, (even.slot, odd.slot), sources, acc, lcat, rcat, mixed, fetch)
    if first:
        lax.fori_loop(ready, channels, fetch, None)


def finish(place, x, total):
    keep = place.keep(x.shape, 0) & place.is_allowed()
    return jnp.where(keep, x.astype(jnp.float32) - TIME_STEP * total, 0.0).astype(jnp.bfloat16)


def split_kernel(x, even, odd, even_sem, odd_sem):
    maxs = even.shape[0]
    odd_col = lax.rem(lax.axis_index("right"), 2)
    copies = [
        pltpu.make_async_copy(x.at[pl.ds(pl.multiple_of(slot * maxs, maxs), maxs)], block, sem)
        for slot, block, sem in ((odd_col, even, even_sem), (1 - odd_col, odd, odd_sem))
    ]
    for copy in copies:
        copy.start()
    for copy in copies:
        copy.wait()


def far_kernel(stream, first, last, ls, rs, al, sh, x, acc_in, left, right, *rest):
    place = Place((ls, rs, al, sh), stream)
    count = 2 if stream == "even" else 1
    halos = rest[:count]
    out, acc, sources, mixed, list_ref = rest[-5:]
    shifts = (place.far_shift, -place.far_shift)[:count]
    for i, (halo, shift) in enumerate(zip(halos, shifts)):
        sources[i] = place.masked(halo[...], shift) if first else halo[...]
    acc[0] = acc_in[0 if stream == "even" else 1]
    tasks = Tasks(place, list_ref)
    tasks.add(2, ((place, 0, 0),))
    if count == 2:
        tasks.add(1, ((place, 1, 0),))
    add_channels(tasks, (place.slot, place.slot), sources, acc, left, right, mixed)
    new = finish(place, x[...], acc[0])
    if last and stream == "even":
        maxs = x.shape[0]
        out[pl.ds(pl.multiple_of(place.slot * maxs, maxs), maxs), :] = new
        out[pl.ds(pl.multiple_of((1 - place.slot) * maxs, maxs), maxs), :] = rest[count][...]
    else:
        out[...] = new


def body(wavefunction, left_env, right_env, left_sizes, right_sizes, allowed, channel_shift):
    channels, local_rows, maxs = left_env.shape
    rows, cols = lax.axis_size("left"), lax.axis_size("right")
    assert local_rows == 2 * maxs and wavefunction.shape == (local_rows, maxs)
    block = jax.ShapeDtypeStruct((maxs, maxs), jnp.bfloat16)
    total = jax.ShapeDtypeStruct((2, maxs, maxs), jnp.float32)
    smem = pl.BlockSpec(memory_space=pltpu.SMEM)
    vmem = pl.BlockSpec(memory_space=pltpu.VMEM)
    hbm = pl.BlockSpec(memory_space=pltpu.HBM)
    sizes = (left_sizes, right_sizes, allowed, channel_shift)
    wavefunction = pltpu.with_memory_space_constraint(wavefunction, pltpu.HBM)
    left_env = pltpu.with_memory_space_constraint(left_env, pltpu.HBM)
    right_env = pltpu.with_memory_space_constraint(right_env, pltpu.HBM)

    def call(kernel, items, ins, outs, scratch, name, env=vmem):
        specs = [env if a is left_env or a is right_env else vmem for a in ins]
        return pl.pallas_call(
            kernel,
            in_specs=[smem] * 4 + specs,
            out_specs=jax.tree.map(lambda _: vmem, outs),
            out_shape=outs,
            scratch_shapes=scratch,
            cost_estimate=pl.CostEstimate(flops=int(items * 4 * maxs**3), bytes_accessed=0, transcendentals=0),
            compiler_params=pltpu.CompilerParams(vmem_limit_bytes=10 << 20),
            name=name,
        )(*sizes, *ins)

    xe, xo = pl.pallas_call(
        split_kernel,
        in_specs=[hbm],
        out_specs=(vmem, vmem),
        out_shape=(block, block),
        scratch_shapes=[pltpu.SemaphoreType.DMA, pltpu.SemaphoreType.DMA],
        compiler_params=pltpu.CompilerParams(vmem_limit_bytes=4 << 20),
        name="split",
    )(wavefunction)
    pairs = functools.partial(permute_pairs, rows, cols)
    mixed = pltpu.VMEM((2 * maxs, maxs), jnp.bfloat16)
    listing = pltpu.SMEM((4, 2 * channels), jnp.int32)
    left_cat, right_cat = left_env, right_env
    for step in range(STEPS):
        first, last = step == 0, step == STEPS - 1
        e_side = lax.ppermute(xe, AXES, pairs((0, -1), (0, 1)))
        o_near = lax.ppermute(xo, AXES, pairs((0, 1), (0, -1)))
        e_up = lax.ppermute(xe, AXES, pairs((-1, 1), (1, -1)))
        o_far = lax.ppermute(xo, AXES, pairs((1, -1), (-1, 1)))
        scratch = [pltpu.VMEM((3, maxs, maxs), jnp.bfloat16), mixed, listing]
        if first:
            sems = [pltpu.SemaphoreType.DMA((channels,))] * 2
            acc, left_cat, right_cat = call(
                functools.partial(near_kernel, True),
                channels,
                (xe, xo, o_near, left_env, right_env),
                (
                    total,
                    pltpu.VMEM((local_rows, channels * maxs), jnp.bfloat16),
                    pltpu.VMEM((maxs, channels * maxs), jnp.bfloat16),
                ),
                scratch + [pltpu.SMEM((channels,), jnp.int32)] + sems,
                "near0",
                hbm,
            )
            left_cat = pltpu.with_memory_space_constraint(left_cat, pltpu.VMEM)
            right_cat = pltpu.with_memory_space_constraint(right_cat, pltpu.VMEM)
        else:
            acc = call(
                functools.partial(near_kernel, False),
                channels,
                (xe, xo, o_near, left_cat, right_cat),
                total,
                scratch,
                "near%d" % step,
            )
        acc_scratch = pltpu.VMEM((1, maxs, maxs), jnp.float32)
        new_o = call(
            functools.partial(far_kernel, "odd", first, last),
            channels / 3,
            (xo, acc, left_cat, right_cat, o_far),
            block,
            [acc_scratch, pltpu.VMEM((1, maxs, maxs), jnp.bfloat16), mixed, listing],
            "odd%d" % step,
        )
        new_e = call(
            functools.partial(far_kernel, "even", first, last),
            channels / 2,
            (xe, acc, left_cat, right_cat, e_side, e_up) + ((new_o,) if last else ()),
            jax.ShapeDtypeStruct(wavefunction.shape, jnp.bfloat16) if last else block,
            [acc_scratch, pltpu.VMEM((2, maxs, maxs), jnp.bfloat16), mixed, listing],
            "even%d" % step,
        )
        xe, xo = new_e, new_o
    return xe


def solution(mesh):
    in_specs = (
        P("left", "right"),
        P(None, "left", None),
        P(None, None, "right"),
        P(),
        P(),
        P(),
        P(),
    )
    out_specs = P("left", "right")
    return jax.shard_map(body, mesh=mesh, in_specs=in_specs, out_specs=out_specs, check_vma=False)
```
